16 devices in a mesh: ep: 16 (over z, y, x, core).
Axes of the slice: x: 2, y: 2, z: 2, core: 2. Of those that a mesh axis runs over, the one named last changes fastest.
Arguments:
- x_in: bfloat16 [8192, 2560], P('ep')
- route_idx: int32 [8192, 6], P('ep')
- gate_w: bfloat16 [8192, 6], P('ep')
- dy_in: bfloat16 [8192, 2560], P('ep')
- w_gate: bfloat16 [16, 2560, 1536], P('ep')
- w_up: bfloat16 [16, 2560, 1536], P('ep')
- w_down: bfloat16 [16, 1536, 2560], P('ep')
- hot_gate: bfloat16 [2560, 1536], replicated
- hot_up: bfloat16 [2560, 1536], replicated
- hot_down: bfloat16 [1536, 2560], replicated
Outputs:
- output 1: bfloat16 [8192, 2560], P('ep')
- output 2: bfloat16 [8192, 2560], P('ep')
- output 3: float32 [16, 2560, 1536], P('ep')
- output 4: float32 [16, 2560, 1536], P('ep')
- output 5: float32 [16, 1536, 2560], P('ep')
- output 6: float32 [2560, 1536], P(None, 'ep')
- output 7: float32 [2560, 1536], P(None, 'ep')
- output 8: float32 [1536, 2560], P('ep')
All inputs are finite; a program needn't handle non-finite values.
Results may differ from the reference program's by a relative error of at most 0.00844653.
Values are sent between devices in bfloat16 or wider.
A program may use at most 1 GiB of HBM per device.

```python
import jax
import jax.numpy as jnp
from jax import lax

N_DEV = 16
TOK_DEV = 512
D_MODEL = 2560
D_FF = 1536
TOP_K = 6

SLOT_CAP = min(TOK_DEV, 2 * TOK_DEV * TOP_K // N_DEV)
HOT_CAP = 3 * TOK_DEV // 4
TOTAL = N_DEV * TOK_DEV


def draw_routes(rng_key):
    heavy_key, weight_key, hot_key, pick_key, order_key, shift_key = jax.random.split(rng_key, 6)
    expert_ids = jnp.arange(N_DEV, dtype=jnp.int32)
    heavy = jax.random.randint(heavy_key, (N_DEV,), 0, N_DEV)
    is_heavy = expert_ids[None, :] == heavy[:, None]
    weight = jnp.where(is_heavy, 0, jax.random.randint(weight_key, (N_DEV, N_DEV), 1, 9))
    hot_count = jax.random.randint(hot_key, (N_DEV,), HOT_CAP // 4, HOT_CAP + 1)
    hot_count = jnp.where(expert_ids == jax.random.randint(pick_key, (), 0, N_DEV), HOT_CAP, hot_count)
    rest = TOK_DEV * TOP_K - hot_count - SLOT_CAP
    base = jnp.minimum((rest[:, None] * weight) // jnp.sum(weight, axis=1, keepdims=True), SLOT_CAP)
    room = jnp.where(is_heavy, 0, SLOT_CAP - base)
    deficit = rest - jnp.sum(base, axis=1)
    before = jnp.cumsum(room, axis=1) - room
    extra = jnp.minimum(jnp.maximum(deficit[:, None] - before, 0), room)
    load = base + extra + jnp.where(is_heavy, SLOT_CAP, 0)
    bounds = jnp.cumsum(jnp.concatenate([load, hot_count[:, None]], axis=1), axis=1)
    positions = jnp.arange(TOK_DEV * TOP_K, dtype=jnp.int32)
    ordered = jax.vmap(lambda bound_row: jnp.searchsorted(bound_row, positions, side='right'))(bounds)
    grid = ordered.reshape(N_DEV, TOP_K, TOK_DEV).transpose(0, 2, 1)
    token_order = jax.vmap(lambda sub_key: jax.random.permutation(sub_key, TOK_DEV))(jax.random.split(order_key, N_DEV))
    grid = jnp.take_along_axis(grid, token_order[:, :, None], axis=1)
    shift = jax.random.randint(shift_key, (N_DEV, TOK_DEV, 1), 0, TOP_K)
    col_index = (jnp.arange(TOP_K, dtype=jnp.int32)[None, None, :] + shift) % TOP_K
    grid = jnp.take_along_axis(grid, col_index, axis=2)
    return grid.reshape(TOTAL, TOP_K).astype(jnp.int32)


def setup_inputs(seed: int = 0) -> dict:
    sub_keys = jax.random.split(jax.random.key(seed), 10)
    in_scale = D_MODEL ** -0.5
    hid_scale = D_FF ** -0.5
    x_in = jax.random.normal(sub_keys[0], (TOTAL, D_MODEL), jnp.float32).astype(jnp.bfloat16)
    route_idx = draw_routes(sub_keys[1])
    gate_w = jax.random.uniform(sub_keys[2], (TOTAL, TOP_K), jnp.float32, 0.5, 1.5).astype(jnp.bfloat16)
    dy_in = jax.random.normal(sub_keys[3], (TOTAL, D_MODEL), jnp.float32).astype(jnp.bfloat16)
    w_gate = (jax.random.normal(sub_keys[4], (N_DEV, D_MODEL, D_FF), jnp.float32) * in_scale).astype(jnp.bfloat16)
    w_up = (jax.random.normal(sub_keys[5], (N_DEV, D_MODEL, D_FF), jnp.float32) * in_scale).astype(jnp.bfloat16)
    w_down = (jax.random.normal(sub_keys[6], (N_DEV, D_FF, D_MODEL), jnp.float32) * hid_scale).astype(jnp.bfloat16)
    hot_gate = (jax.random.normal(sub_keys[7], (D_MODEL, D_FF), jnp.float32) * in_scale).astype(jnp.bfloat16)
    hot_up = (jax.random.normal(sub_keys[8], (D_MODEL, D_FF), jnp.float32) * in_scale).astype(jnp.bfloat16)
    hot_down = (jax.random.normal(sub_keys[9], (D_FF, D_MODEL), jnp.float32) * hid_scale).astype(jnp.bfloat16)
    return {'x_in': x_in, 'route_idx': route_idx, 'gate_w': gate_w, 'dy_in': dy_in, 'w_gate': w_gate, 'w_up': w_up, 'w_down': w_down, 'hot_gate': hot_gate, 'hot_up': hot_up, 'hot_down': hot_down}


def silu_parts(pre_gate):
    sig_val = jax.nn.sigmoid(pre_gate)
    return pre_gate * sig_val, sig_val * (1.0 + pre_gate * (1.0 - sig_val))


def expert_pass(x_rows, d_rows, gate_mat, up_mat, down_mat):
    u_val = jnp.dot(x_rows, gate_mat, preferred_element_type=jnp.float32)
    v_val = jnp.dot(x_rows, up_mat, preferred_element_type=jnp.float32)
    silu_val, silu_grad = silu_parts(u_val)
    hidden = (silu_val * v_val).astype(jnp.bfloat16)
    result = jnp.dot(hidden, down_mat, preferred_element_type=jnp.float32).astype(jnp.bfloat16)
    grad_hidden = jnp.dot(d_rows, down_mat.T, preferred_element_type=jnp.float32).astype(jnp.bfloat16).astype(jnp.float32)
    grad_u = (grad_hidden * v_val * silu_grad).astype(jnp.bfloat16)
    grad_v = (grad_hidden * silu_val).astype(jnp.bfloat16)
    grad_x = (jnp.dot(grad_u, gate_mat.T, preferred_element_type=jnp.float32) + jnp.dot(grad_v, up_mat.T, preferred_element_type=jnp.float32)).astype(jnp.bfloat16)
    grad_gate = jnp.dot(x_rows.T, grad_u, preferred_element_type=jnp.float32)
    grad_up = jnp.dot(x_rows.T, grad_v, preferred_element_type=jnp.float32)
    grad_down = jnp.dot(hidden.T, d_rows, preferred_element_type=jnp.float32)
    return result, grad_x, (grad_gate, grad_up, grad_down)


def reference(x_in, route_idx, gate_w, dy_in, w_gate, w_up, w_down, hot_gate, hot_up, hot_down):
    flat_ids = route_idx.reshape(-1)
    n_assign = flat_ids.shape[0]
    order = jnp.argsort(flat_ids, stable=True)
    starts = jnp.searchsorted(flat_ids[order], jnp.arange(N_DEV + 2, dtype=jnp.int32), side='left')
    gate_flat = gate_w.reshape(-1)

    def take_block(first, last, max_rows):
        position = first + jnp.arange(max_rows, dtype=jnp.int32)
        assign = jnp.where(position < last, order[jnp.minimum(position, n_assign - 1)], n_assign)
        token = assign // TOP_K
        x_rows = jnp.take(x_in, token, axis=0, mode='fill', fill_value=0)
        gate_rows = jnp.take(gate_flat, assign, mode='fill', fill_value=0).astype(jnp.float32)
        dy_rows = jnp.take(dy_in, token, axis=0, mode='fill', fill_value=0).astype(jnp.float32)
        d_rows = (gate_rows[:, None] * dy_rows).astype(jnp.bfloat16)
        return token, gate_rows, x_rows, d_rows

    def add_block(sums, token, gate_rows, result, grad_x):
        y_sum, dx_sum = sums
        y_sum = y_sum.at[token].add(gate_rows[:, None] * result.astype(jnp.float32), mode='drop')
        dx_sum = dx_sum.at[token].add(grad_x.astype(jnp.float32), mode='drop')
        return y_sum, dx_sum

    def regular_step(sums, expert_args):
        gate_mat, up_mat, down_mat, first, last = expert_args
        token, gate_rows, x_rows, d_rows = take_block(first, last, N_DEV * SLOT_CAP)
        result, grad_x, grads = expert_pass(x_rows, d_rows, gate_mat, up_mat, down_mat)
        return add_block(sums, token, gate_rows, result, grad_x), grads

    zero_sum = jnp.zeros((TOTAL, D_MODEL), jnp.float32)
    sums, (dw_gate, dw_up, dw_down) = lax.scan(regular_step, (zero_sum, zero_sum), (w_gate, w_up, w_down, starts[:N_DEV], starts[1:N_DEV + 1]))
    token, gate_rows, x_rows, d_rows = take_block(starts[N_DEV], starts[N_DEV + 1], N_DEV * HOT_CAP)
    result, grad_x, (dhot_gate, dhot_up, dhot_down) = expert_pass(x_rows, d_rows, hot_gate, hot_up, hot_down)
    y_sum, dx_sum = add_block(sums, token, gate_rows, result, grad_x)
    return (y_sum.astype(jnp.bfloat16), dx_sum.astype(jnp.bfloat16), dw_gate, dw_up, dw_down, dhot_gate, dhot_up, dhot_down)
```

```python
import jax
import jax.numpy as jnp
from jax import lax
from jax.sharding import PartitionSpec as P

CONTRACT_LAST = (((1,), (1,)), ((), ()))
CONTRACT_FIRST = (((0,), (0,)), ((), ()))


def silu_parts(pre_gate):
    sig_val = jax.nn.sigmoid(pre_gate)
    return pre_gate * sig_val, sig_val * (1.0 + pre_gate * (1.0 - sig_val))


def dot_f32(lhs, rhs, dims=(((1,), (0,)), ((), ()))):
    return lax.dot_general(lhs, rhs, dims, preferred_element_type=jnp.float32)


def expert_forward(x_rows, gate_mat, up_mat, down_mat):
    u_val = dot_f32(x_rows, gate_mat)
    v_val = dot_f32(x_rows, up_mat)
    silu_val, silu_grad = silu_parts(u_val)
    hidden = (silu_val * v_val).astype(jnp.bfloat16)
    result = dot_f32(hidden, down_mat).astype(jnp.bfloat16)
    return result, hidden, v_val, silu_val, silu_grad


def hidden_grads(d_rows, v_val, silu_val, silu_grad, down_mat):
    grad_hidden = dot_f32(d_rows, down_mat, CONTRACT_LAST).astype(jnp.bfloat16).astype(jnp.float32)
    grad_u = (grad_hidden * v_val * silu_grad).astype(jnp.bfloat16)
    grad_v = (grad_hidden * silu_val).astype(jnp.bfloat16)
    return grad_u, grad_v


def input_grad(grad_u, grad_v, gate_mat, up_mat):
    return (dot_f32(grad_u, gate_mat, CONTRACT_LAST) + dot_f32(grad_v, up_mat, CONTRACT_LAST)).astype(jnp.bfloat16)


def scaled(gate_col, rows):
    return (gate_col.astype(jnp.float32)[:, None] * rows.astype(jnp.float32)).astype(jnp.bfloat16)


def solution(mesh):
    n_dev = mesh.shape['ep']

    def local_step(x_loc, route_loc, gate_loc, dy_loc, w_gate, w_up, w_down, hot_gate, hot_up, hot_down):
        tok_rows, top_k = route_loc.shape
        d_model = x_loc.shape[1]
        d_ff = hot_gate.shape[1]
        part = d_ff // n_dev
        slot_cap = min(tok_rows, 2 * tok_rows * top_k // n_dev)
        w_gate, w_up, w_down = w_gate[0], w_up[0], w_down[0]
        me = lax.axis_index('ep')

        x_all = lax.all_gather(x_loc, 'ep', axis=0, tiled=True)
        dy_all = lax.all_gather(dy_loc, 'ep', axis=0, tiled=True)

        experts = jnp.arange(n_dev + 1, dtype=jnp.int32)
        picks = route_loc[:, :, None] == experts[None, None, :]
        gates = jnp.sum(jnp.where(picks, gate_loc.astype(jnp.float32)[:, :, None], 0.0), axis=1)
        member = jnp.any(picks, axis=1)
        token_ids = jnp.arange(tok_rows, dtype=jnp.int32)
        earlier = (token_ids[:, None] > token_ids[None, :]).astype(jnp.bfloat16)
        rank = dot_f32(earlier, member.astype(jnp.bfloat16))
        gate_hot = gates[:, n_dev]

        slot_rank = jnp.where(member, rank, -1.0)[:, :n_dev].T
        table = jnp.concatenate([slot_rank, gates[:, :n_dev].T, jnp.broadcast_to(gate_hot[None, :], (n_dev, tok_rows))], axis=1)
        table = lax.all_to_all(table, 'ep', 0, 0, tiled=True)
        rank_in = table[:, :tok_rows]
        gate_in = table[:, tok_rows:2 * tok_rows].astype(jnp.bfloat16)
        hot_in = table[:, 2 * tok_rows:3 * tok_rows].reshape(-1)

        out_hot, _, v_hot, silu_hot, sgrad_hot = expert_forward(x_loc, hot_gate, hot_up, hot_down)
        du_hot, dv_hot = hidden_grads(scaled(gate_hot, dy_loc), v_hot, silu_hot, sgrad_hot, hot_down)
        dx_hot = input_grad(du_hot, dv_hot, hot_gate, hot_up)

        x_all, out_hot, dx_hot = lax.optimization_barrier((x_all, out_hot, dx_hot))
        slots = jnp.arange(slot_cap, dtype=jnp.float32)
        match = rank_in[:, None, :] == slots[None, :, None]
        batched = (((2,), (1,)), ((0,), (0,)))
        x_rows = dot_f32(match.astype(jnp.bfloat16), x_all.reshape(n_dev, tok_rows, d_model), batched)
        x_rows = x_rows.astype(jnp.bfloat16).reshape(-1, d_model)
        out_rows, hidden, v_val, silu_val, silu_grad = expert_forward(x_rows, w_gate, w_up, w_down)

        def send_back(rows):
            return lax.all_to_all(rows, 'ep', 0, 0, tiled=True)

        out_rows, dy_all = lax.optimization_barrier((out_rows, dy_all))
        out_back = send_back(out_rows)

        q_match = jnp.where(match, gate_in[:, None, :], jnp.bfloat16(0))
        q_rows = dot_f32(q_match, dy_all.reshape(n_dev, tok_rows, d_model), batched)
        q_rows = q_rows.astype(jnp.bfloat16).reshape(-1, d_model)
        du_val, dv_val = hidden_grads(q_rows, v_val, silu_val, silu_grad, w_down)
        dx_rows = input_grad(du_val, dv_val, w_gate, w_up)
        dx_rows, x_rows, hidden, q_rows, du_val, dv_val = lax.optimization_barrier((dx_rows, x_rows, hidden, q_rows, du_val, dv_val))
        dx_back = send_back(dx_rows)
        grad_gate = dot_f32(x_rows, du_val, CONTRACT_FIRST)
        grad_up = dot_f32(x_rows, dv_val, CONTRACT_FIRST)
        grad_down = dot_f32(hidden, q_rows, CONTRACT_FIRST)

        first_unit = me * part
        hg = lax.dynamic_slice_in_dim(hot_gate, first_unit, part, 1)
        hu = lax.dynamic_slice_in_dim(hot_up, first_unit, part, 1)
        hd = lax.dynamic_slice_in_dim(hot_down, first_unit, part, 0)
        uv = dot_f32(x_all, jnp.concatenate([hg, hu], axis=1))
        silu_p, sgrad_p = silu_parts(uv[:, :part])
        v_p = uv[:, part:]
        hid_p = (silu_p * v_p).astype(jnp.bfloat16)
        q_all = scaled(hot_in, dy_all)
        du_p, dv_p = hidden_grads(q_all, v_p, silu_p, sgrad_p, hd)
        dguh = dot_f32(x_all, jnp.concatenate([du_p, dv_p], axis=1), CONTRACT_FIRST)
        hot_ddown = dot_f32(hid_p, q_all, CONTRACT_FIRST)

        regular = picks[:, :, :n_dev]
        place = jnp.arange(n_dev, dtype=jnp.float32)[None, :] * slot_cap + rank[:, :n_dev]
        dest = jnp.sum(jnp.where(regular, place[:, None, :] + 1.0, 0.0), axis=2) - 1.0
        row_ids = jnp.arange(n_dev * slot_cap, dtype=jnp.float32)
        hits = dest[:, :, None] == row_ids[None, None, :]
        gate_mix = jnp.sum(jnp.where(hits, gate_loc.astype(jnp.float32)[:, :, None], 0.0), axis=1).astype(jnp.bfloat16)
        plain_mix = jnp.any(hits, axis=1).astype(jnp.bfloat16)
        y_loc = dot_f32(gate_mix, out_back) + gate_hot[:, None] * out_hot.astype(jnp.float32)
        dx_loc = dot_f32(plain_mix, dx_back) + dx_hot.astype(jnp.float32)
        return (y_loc.astype(jnp.bfloat16), dx_loc.astype(jnp.bfloat16), grad_gate[None], grad_up[None], grad_down[None],
                dguh[:, :part], dguh[:, part:], hot_ddown)

    row_spec = P('ep', None)
    expert_spec = P('ep', None, None)
    whole_spec = P(None, None)
    return jax.shard_map(local_step, mesh=mesh, in_specs=(row_spec, row_spec, row_spec, row_spec, expert_spec, expert_spec, expert_spec, whole_spec, whole_spec, whole_spec), out_specs=(row_spec, row_spec, expert_spec, expert_spec, expert_spec, P(None, 'ep'), P(None, 'ep'), P('ep', None)), check_vma=False)
```

```python
import jax
import jax.numpy as jnp
from jax import lax
from jax.sharding import PartitionSpec as P


CONTRACT_LAST = (((1,), (1,)), ((), ()))
CONTRACT_FIRST = (((0,), (0,)), ((), ()))


def silu_parts(pre_gate):
    sig_val = jax.nn.sigmoid(pre_gate)
    return pre_gate * sig_val, sig_val * (1.0 + pre_gate * (1.0 - sig_val))


def dot_f32(lhs, rhs, dims=(((1,), (0,)), ((), ()))):
    return lax.dot_general(lhs, rhs, dims, preferred_element_type=jnp.float32)


def expert_forward(x_rows, gate_mat, up_mat, down_mat):
    u_val = dot_f32(x_rows, gate_mat)
    v_val = dot_f32(x_rows, up_mat)
    silu_val, silu_grad = silu_parts(u_val)
    hidden = (silu_val * v_val).astype(jnp.bfloat16)
    result = dot_f32(hidden, down_mat).astype(jnp.bfloat16)
    return result, hidden, v_val, silu_val, silu_grad


def hidden_grads(d_rows, v_val, silu_val, silu_grad, down_mat):
    grad_hidden = lax.reduce_precision(dot_f32(d_rows, down_mat, CONTRACT_LAST), 8, 7)
    grad_u = (grad_hidden * v_val * silu_grad).astype(jnp.bfloat16)
    grad_v = (grad_hidden * silu_val).astype(jnp.bfloat16)
    return grad_u, grad_v


def input_grad(grad_u, grad_v, gate_mat, up_mat):
    return (dot_f32(grad_u, gate_mat, CONTRACT_LAST) + dot_f32(grad_v, up_mat, CONTRACT_LAST)).astype(jnp.bfloat16)


def scaled(gate_col, rows):
    return (gate_col.astype(jnp.float32)[:, None] * rows.astype(jnp.float32)).astype(jnp.bfloat16)


def solution(mesh):
    n_dev = mesh.shape['ep']

    def local_body(x_loc, route_loc, gate_loc, dy_loc, w_gate, w_up, w_down, hot_gate, hot_up, hot_down):
        tok_rows, top_k = route_loc.shape
        d_model = x_loc.shape[1]
        d_ff = hot_gate.shape[1]
        part = d_ff // n_dev
        slot_cap = min(tok_rows, 2 * tok_rows * top_k // n_dev)
        w_gate, w_up, w_down = w_gate[0], w_up[0], w_down[0]
        me = lax.axis_index('ep')

        x_all = lax.all_gather(x_loc, 'ep', axis=0, tiled=True)
        dy_all = lax.all_gather(dy_loc, 'ep', axis=0, tiled=True)

        experts = jnp.arange(n_dev + 1, dtype=jnp.int32)
        picks = route_loc[:, :, None] == experts[None, None, :]
        gates = jnp.sum(jnp.where(picks, gate_loc.astype(jnp.float32)[:, :, None], 0.0), axis=1)
        member = jnp.any(picks, axis=1)
        token_ids = jnp.arange(tok_rows, dtype=jnp.int32)
        earlier = (token_ids[:, None] > token_ids[None, :]).astype(jnp.bfloat16)
        rank = dot_f32(earlier, member.astype(jnp.bfloat16))
        gate_hot = gates[:, n_dev]

        slot_rank = jnp.where(member, rank, -1.0)[:, :n_dev].T
        table = jnp.concatenate([slot_rank, gates[:, :n_dev].T, jnp.broadcast_to(gate_hot[None, :], (n_dev, tok_rows))], axis=1)
        table = lax.all_to_all(table, 'ep', 0, 0, tiled=True)
        rank_in = table[:, :tok_rows]
        gate_in = table[:, tok_rows:2 * tok_rows].astype(jnp.bfloat16)
        hot_in = table[:, 2 * tok_rows:3 * tok_rows].reshape(-1)

        out_hot, _, v_hot, silu_hot, sgrad_hot = expert_forward(x_loc, hot_gate, hot_up, hot_down)
        du_hot, dv_hot = hidden_grads(scaled(gate_hot, dy_loc), v_hot, silu_hot, sgrad_hot, hot_down)
        dx_hot = input_grad(du_hot, dv_hot, hot_gate, hot_up)

        cuts = (0, slot_cap // 3, slot_cap)
        chunks = tuple(zip(cuts[:-1], cuts[1:]))
        regular = picks[:, :, :n_dev]
        mixes = []
        for low, high in chunks:
            inside = (rank[:, :n_dev] >= low) & (rank[:, :n_dev] < high)
            place = jnp.arange(n_dev, dtype=jnp.float32)[None, :] * (high - low) + (rank[:, :n_dev] - low)
            dest = jnp.sum(jnp.where(regular & inside[:, None, :], place[:, None, :] + 1.0, 0.0), axis=2) - 1.0
            hits = dest[:, :, None] == jnp.arange(n_dev * (high - low), dtype=jnp.float32)[None, None, :]
            gate_mix = jnp.sum(jnp.where(hits, gate_loc.astype(jnp.float32)[:, :, None], 0.0), axis=1).astype(jnp.bfloat16)
            mixes.append((gate_mix, jnp.any(hits, axis=1).astype(jnp.bfloat16)))

        x_all, out_hot, dx_hot, mixes = lax.optimization_barrier((x_all, out_hot, dx_hot, mixes))
        batched = (((2,), (1,)), ((0,), (0,)))

        def match_of(low, high):
            return rank_in[:, None, :] == jnp.arange(low, high, dtype=jnp.float32)[None, :, None]

        def pick(weights, rows):
            got = dot_f32(weights, rows.reshape(n_dev, tok_rows, d_model), batched)
            return got.astype(jnp.bfloat16).reshape(-1, d_model)

        def send_back(rows):
            return lax.all_to_all(rows, 'ep', 0, 0, tiled=True)

        def forward(bounds, x_all):
            x_rows = pick(match_of(*bounds).astype(jnp.bfloat16), x_all)
            return x_rows, expert_forward(x_rows, w_gate, w_up, w_down)

        def backward(bounds, dy_all, saved):
            q_rows = pick(jnp.where(match_of(*bounds), gate_in[:, None, :], jnp.bfloat16(0)), dy_all)
            du_val, dv_val = hidden_grads(q_rows, *saved, w_down)
            return q_rows, du_val, dv_val, input_grad(du_val, dv_val, w_gate, w_up)

        x_a, (out_a, hidden_a, *saved_a) = forward(chunks[0], x_all)
        out_a, x_all = lax.optimization_barrier((out_a, x_all))
        out_back_a = send_back(out_a)
        x_b, (out_b, hidden_b, *saved_b) = forward(chunks[1], x_all)
        order = lax.optimization_barrier
        out_back_a, out_b, dy_all, x_all = order((out_back_a, out_b, dy_all, x_all))
        out_back_b = send_back(out_b)
        q_b, du_b, dv_b, dx_b = backward(chunks[1], dy_all, saved_b)
        dx_b, x_all, dy_all = order((dx_b, x_all, dy_all))

        first_unit = me * part
        hg = lax.dynamic_slice_in_dim(hot_gate, first_unit, part, 1)
        hu = lax.dynamic_slice_in_dim(hot_up, first_unit, part, 1)
        hd = lax.dynamic_slice_in_dim(hot_down, first_unit, part, 0)
        uv = dot_f32(x_all, jnp.concatenate([hg, hu], axis=1))
        silu_p, sgrad_p = silu_parts(uv[:, :part])
        v_p = uv[:, part:]
        hid_p = (silu_p * v_p).astype(jnp.bfloat16)
        q_all = scaled(hot_in, dy_all)
        du_p, dv_p = hidden_grads(q_all, v_p, silu_p, sgrad_p, hd)
        dguh = dot_f32(x_all, jnp.concatenate([du_p, dv_p], axis=1), CONTRACT_FIRST)
        hot_ddown = dot_f32(hid_p, q_all, CONTRACT_FIRST)

        out_back_b, dx_b, dguh, hot_ddown, dy_all = order((out_back_b, dx_b, dguh, hot_ddown, dy_all))
        dx_back_b = send_back(dx_b)

        def both(rows_a, grads_a, rows_b, grads_b):
            return dot_f32(rows_b, grads_b, CONTRACT_FIRST) + dot_f32(rows_a, grads_a, CONTRACT_FIRST)

        q_a, du_a, dv_a, dx_a = backward(chunks[0], dy_all, saved_a)
        grad_down = both(hidden_a, q_a, hidden_b, q_b)
        grad_up = both(x_a, dv_a, x_b, dv_b)
        dx_back_b, dx_a, grad_down, grad_up, du_a, du_b, out_back_a, out_back_b = order(
            (dx_back_b, dx_a, grad_down, grad_up, du_a, du_b, out_back_a, out_back_b))
        dx_back_a = send_back(dx_a)
        grad_gate = both(x_a, du_a, x_b, du_b)

        (gate_mix_a, plain_mix_a), (gate_mix_b, plain_mix_b) = mixes
        y_loc = dot_f32(gate_mix_b, out_back_b) + dot_f32(gate_mix_a, out_back_a) + gate_hot[:, None] * out_hot.astype(jnp.float32)
        dx_part = dot_f32(plain_mix_b, dx_back_b) + dx_hot.astype(jnp.float32)
        dx_part = lax.optimization_barrier(dx_part)
        dx_loc = dot_f32(plain_mix_a, dx_back_a) + dx_part
        return (y_loc.astype(jnp.bfloat16), dx_loc.astype(jnp.bfloat16), grad_gate[None], grad_up[None], grad_down[None],
                dguh[:, :part], dguh[:, part:], hot_ddown)

    row_spec = P('ep', None)
    expert_spec = P('ep', None, None)
    whole_spec = P(None, None)
    return jax.shard_map(local_body, mesh=mesh, in_specs=(row_spec, row_spec, row_spec, row_spec, expert_spec, expert_spec, expert_spec, whole_spec, whole_spec, whole_spec), out_specs=(row_spec, row_spec, expert_spec, expert_spec, expert_spec, P(None, 'ep'), P(None, 'ep'), P('ep', None)), check_vma=False)
```

```python
import jax
import jax.numpy as jnp
from jax import lax
from jax.sharding import PartitionSpec as P


CONTRACT_LAST = (((1,), (1,)), ((), ()))
CONTRACT_FIRST = (((0,), (0,)), ((), ()))


def silu_parts(pre_gate):
    sig_val = jax.nn.sigmoid(pre_gate)
    return pre_gate * sig_val, sig_val * (1.0 + pre_gate * (1.0 - sig_val))


def dot_f32(lhs, rhs, dims=(((1,), (0,)), ((), ()))):
    return lax.dot_general(lhs, rhs, dims, preferred_element_type=jnp.float32)


def expert_forward(x_rows, gate_mat, up_mat, down_mat):
    u_val = dot_f32(x_rows, gate_mat)
    v_val = dot_f32(x_rows, up_mat)
    silu_val, silu_grad = silu_parts(u_val)
    hidden = (silu_val * v_val).astype(jnp.bfloat16)
    result = dot_f32(hidden, down_mat).astype(jnp.bfloat16)
    return result, hidden, v_val, silu_val, silu_grad


def hidden_grads(d_rows, v_val, silu_val, silu_grad, down_mat):
    grad_hidden = lax.reduce_precision(dot_f32(d_rows, down_mat, CONTRACT_LAST), 8, 7)
    grad_u = (grad_hidden * v_val * silu_grad).astype(jnp.bfloat16)
    grad_v = (grad_hidden * silu_val).astype(jnp.bfloat16)
    return grad_u, grad_v


def input_grad(grad_u, grad_v, gate_mat, up_mat):
    return (dot_f32(grad_u, gate_mat, CONTRACT_LAST) + dot_f32(grad_v, up_mat, CONTRACT_LAST)).astype(jnp.bfloat16)


def scaled(gate_col, rows):
    return (gate_col.astype(jnp.float32)[:, None] * rows.astype(jnp.float32)).astype(jnp.bfloat16)


def solution(mesh):
    n_dev = mesh.shape['ep']

    def local_body(x_loc, route_loc, gate_loc, dy_loc, w_gate, w_up, w_down, hot_gate, hot_up, hot_down):
        tok_rows, top_k = route_loc.shape
        d_model = x_loc.shape[1]
        d_ff = hot_gate.shape[1]
        part = d_ff // n_dev
        slot_cap = min(tok_rows, 2 * tok_rows * top_k // n_dev)
        w_gate, w_up, w_down = w_gate[0], w_up[0], w_down[0]
        me = lax.axis_index('ep')

        x_all = lax.all_gather(x_loc, 'ep', axis=0, tiled=True)
        dy_all = lax.all_gather(dy_loc, 'ep', axis=0, tiled=True)

        experts = jnp.arange(n_dev + 1, dtype=jnp.int32)
        picks = route_loc[:, :, None] == experts[None, None, :]
        gates = jnp.sum(jnp.where(picks, gate_loc.astype(jnp.float32)[:, :, None], 0.0), axis=1)
        member = jnp.any(picks, axis=1)
        token_ids = jnp.arange(tok_rows, dtype=jnp.int32)
        earlier = (token_ids[:, None] > token_ids[None, :]).astype(jnp.bfloat16)
        rank = dot_f32(earlier, member.astype(jnp.bfloat16))
        gate_hot = gates[:, n_dev]

        slot_rank = jnp.where(member, rank, -1.0)[:, :n_dev].T
        table = jnp.concatenate([slot_rank, gates[:, :n_dev].T, jnp.broadcast_to(gate_hot[None, :], (n_dev, tok_rows))], axis=1)
        table = lax.all_to_all(table, 'ep', 0, 0, tiled=True)
        rank_in = table[:, :tok_rows]
        gate_in = table[:, tok_rows:2 * tok_rows].astype(jnp.bfloat16)
        hot_in = table[:, 2 * tok_rows:3 * tok_rows].reshape(-1)

        out_hot, _, v_hot, silu_hot, sgrad_hot = expert_forward(x_loc, hot_gate, hot_up, hot_down)
        du_hot, dv_hot = hidden_grads(scaled(gate_hot, dy_loc), v_hot, silu_hot, sgrad_hot, hot_down)
        dx_hot = input_grad(du_hot, dv_hot, hot_gate, hot_up)

        cuts = (0, slot_cap // 3, slot_cap)
        chunks = tuple(zip(cuts[:-1], cuts[1:]))
        regular = picks[:, :, :n_dev]
        mixes = []
        for low, high in chunks:
            inside = (rank[:, :n_dev] >= low) & (rank[:, :n_dev] < high)
            place = jnp.arange(n_dev, dtype=jnp.float32)[None, :] * (high - low) + (rank[:, :n_dev] - low)
            dest = jnp.sum(jnp.where(regular & inside[:, None, :], place[:, None, :] + 1.0, 0.0), axis=2) - 1.0
            hits = dest[:, :, None] == jnp.arange(n_dev * (high - low), dtype=jnp.float32)[None, None, :]
            gate_mix = jnp.sum(jnp.where(hits, gate_loc.astype(jnp.float32)[:, :, None], 0.0), axis=1).astype(jnp.bfloat16)
            mixes.append((gate_mix, jnp.any(hits, axis=1).astype(jnp.bfloat16)))

        x_all, out_hot, dx_hot, mixes = lax.optimization_barrier((x_all, out_hot, dx_hot, mixes))
        batched = (((2,), (1,)), ((0,), (0,)))

        def match_of(low, high):
            return rank_in[:, None, :] == jnp.arange(low, high, dtype=jnp.float32)[None, :, None]

        def pick(weights, rows):
            got = dot_f32(weights, rows.reshape(n_dev, tok_rows, d_model), batched)
            return got.astype(jnp.bfloat16).reshape(-1, d_model)

        def send_back(rows):
            return lax.all_to_all(rows, 'ep', 0, 0, tiled=True)

        def swap_back(rows):
            blocks = rows.reshape(n_dev, -1, d_model)
            own = lax.dynamic_slice_in_dim(blocks, me, 1, 0)
            got = lax.dynamic_update_slice_in_dim(jnp.zeros_like(blocks), own, me, 0)
            for step in range(1, n_dev):
                block = lax.dynamic_slice_in_dim(blocks, me ^ step, 1, 0)
                block = lax.ppermute(block, 'ep', [(i, i ^ step) for i in range(n_dev)])
                got = lax.dynamic_update_slice_in_dim(got, block, me ^ step, 0)
            return got.reshape(-1, d_model)

        def forward(bounds, x_all):
            x_rows = pick(match_of(*bounds).astype(jnp.bfloat16), x_all)
            return x_rows, expert_forward(x_rows, w_gate, w_up, w_down)

        def backward(bounds, dy_all, saved):
            q_rows = pick(jnp.where(match_of(*bounds), gate_in[:, None, :], jnp.bfloat16(0)), dy_all)
            du_val, dv_val = hidden_grads(q_rows, *saved, w_down)
            return q_rows, du_val, dv_val, input_grad(du_val, dv_val, w_gate, w_up)

        x_a, (out_a, hidden_a, *saved_a) = forward(chunks[0], x_all)
        out_a, x_all = lax.optimization_barrier((out_a, x_all))
        out_back_a = send_back(out_a)
        x_b, (out_b, hidden_b, *saved_b) = forward(chunks[1], x_all)
        order = lax.optimization_barrier
        out_back_a, out_b, dy_all, x_all = order((out_back_a, out_b, dy_all, x_all))
        out_back_b = send_back(out_b)
        q_a, du_a, dv_a, dx_a = backward(chunks[0], dy_all, saved_a)
        dx_a, dy_all = order((dx_a, dy_all))
        dx_back_a = swap_back(dx_a)
        q_b, du_b, dv_b, dx_b = backward(chunks[1], dy_all, saved_b)
        dx_b, x_all, dy_all = order((dx_b, x_all, dy_all))

        first_unit = me * part
        hg = lax.dynamic_slice_in_dim(hot_gate, first_unit, part, 1)
        hu = lax.dynamic_slice_in_dim(hot_up, first_unit, part, 1)
        hd = lax.dynamic_slice_in_dim(hot_down, first_unit, part, 0)
        uv = dot_f32(x_all, jnp.concatenate([hg, hu], axis=1))
        silu_p, sgrad_p = silu_parts(uv[:, :part])
        v_p = uv[:, part:]
        hid_p = (silu_p * v_p).astype(jnp.bfloat16)
        q_all = scaled(hot_in, dy_all)
        du_p, dv_p = hidden_grads(q_all, v_p, silu_p, sgrad_p, hd)
        dguh = dot_f32(x_all, jnp.concatenate([du_p, dv_p], axis=1), CONTRACT_FIRST)
        hot_ddown = dot_f32(hid_p, q_all, CONTRACT_FIRST)

        out_back_b, dx_b, dguh, hot_ddown, q_a, q_b, du_a, du_b, dv_a, dv_b = order(
            (out_back_b, dx_b, dguh, hot_ddown, q_a, q_b, du_a, du_b, dv_a, dv_b))
        dx_back_b = send_back(dx_b)

        def both(rows_a, grads_a, rows_b, grads_b):
            return dot_f32(rows_b, grads_b, CONTRACT_FIRST) + dot_f32(rows_a, grads_a, CONTRACT_FIRST)

        grad_down = both(hidden_a, q_a, hidden_b, q_b)
        grad_up = both(x_a, dv_a, x_b, dv_b)
        grad_gate = both(x_a, du_a, x_b, du_b)

        (gate_mix_a, plain_mix_a), (gate_mix_b, plain_mix_b) = mixes
        y_loc = dot_f32(gate_mix_b, out_back_b) + dot_f32(gate_mix_a, out_back_a) + gate_hot[:, None] * out_hot.astype(jnp.float32)
        dx_part = dot_f32(plain_mix_a, dx_back_a) + dx_hot.astype(jnp.float32)
        dx_part = lax.optimization_barrier(dx_part)
        dx_loc = dot_f32(plain_mix_b, dx_back_b) + dx_part
        return (y_loc.astype(jnp.bfloat16), dx_loc.astype(jnp.bfloat16), grad_gate[None], grad_up[None], grad_down[None],
                dguh[:, :part], dguh[:, part:], hot_ddown)

    row_spec = P('ep', None)
    expert_spec = P('ep', None, None)
    whole_spec = P(None, None)
    return jax.shard_map(local_body, mesh=mesh, in_specs=(row_spec, row_spec, row_spec, row_spec, expert_spec, expert_spec, expert_spec, whole_spec, whole_spec, whole_spec), out_specs=(row_spec, row_spec, expert_spec, expert_spec, expert_spec, P(None, 'ep'), P(None, 'ep'), P('ep', None)), check_vma=False)
```
